32 devices in a mesh: gx: 4 (over y, core), gy: 8 (over z, x).
Axes of the slice: x: 2, y: 2, z: 4, core: 2. Of those that a mesh axis runs over, the one named last changes fastest.
Arguments:
- transfer: bfloat16 [512, 75, 128], P(('gx', 'gy')), may hold values from -6 to 6
- positions: float32 [512, 3, 128], P(('gx', 'gy')), may hold values from -4 to 4
- normals: float32 [512, 3, 128], P(('gx', 'gy')), may hold values from -4 to 4
- area: float32 [512, 128], P(('gx', 'gy')), may hold values from 0.06 to 3
- albedo: float32 [512, 3, 128], P(('gx', 'gy')), may hold values from 0.3 to 0.9
- pairs: int32 [512, 40], P(('gx', 'gy')), may hold values from 0 to 511, as said below
- home: int32 [512], replicated, may hold values from 0 to 511, as said below
Outputs:
- bounce_one: bfloat16 [512, 75, 128], P(('gx', 'gy'))
- bounce_two: bfloat16 [512, 75, 128], P(('gx', 'gy'))
- energies: float32 [2], replicated
The draws below stay inside these ranges and needn't reach their ends.
Inputs may be any that keep to these rules, and one draw needn't show every extreme that they name: `home`: A permutation; the block in slot s is held by device s // 16, devices counted gx major. `pairs`: the first 16 entries of a row name blocks held by the same device as the row's slot, the other 24 name blocks held by other devices. Over the rows of one device, the far entries name at most 2 distinct blocks of any one other device, and exactly 2 of some. Ids may repeat within a row; each entry counts.
All inputs are finite; a program needn't handle non-finite values.
Results may differ from the reference program's by a relative error of at most 0.02.
Values may be sent and summed in bfloat16 or wider, within the bound.
A program may use at most 128 MiB of HBM per device.

```python
import jax
import jax.numpy as jnp
from jax import lax

BLK_DEV = 16
VERT = 128
COLORS = 3
NEAR = 16
FAR = 24
CAP = 2
CH = 75
BLOCKS = 512


def layout_tables(key):
    devices_all = BLOCKS // BLK_DEV
    home = jax.random.permutation(jax.random.fold_in(key, 11), BLOCKS).astype(jnp.int32)
    inverse = jnp.argsort(home, stable=True).astype(jnp.int32)
    keys = jax.random.split(jax.random.fold_in(key, 12), 4)
    slot_all = jnp.arange(BLOCKS, dtype=jnp.int32)
    device_of = slot_all // BLK_DEV
    near_local = jax.random.randint(keys[0], (BLOCKS, NEAR), 0, BLK_DEV, dtype=jnp.int32)
    near_slot = device_of[:, None] * BLK_DEV + near_local
    offset = jax.random.randint(keys[1], (BLOCKS, FAR), 1, devices_all, dtype=jnp.int32)
    column = jnp.arange(FAR, dtype=jnp.int32)[None, :]
    forced = (slot_all % BLK_DEV == 0)[:, None] & (column < CAP)
    offset = jnp.where(forced, 1, offset)
    pick_k = jax.random.randint(keys[2], (BLOCKS, FAR), 0, CAP, dtype=jnp.int32)
    pick_k = jnp.where(forced, column, pick_k)
    owner_dev = (device_of[:, None] + offset) % devices_all
    start_tab = jax.random.randint(keys[3], (devices_all, devices_all), 0, BLK_DEV, dtype=jnp.int32)
    local_idx = (start_tab[device_of[:, None], owner_dev] + pick_k) % BLK_DEV
    far_slot = owner_dev * BLK_DEV + local_idx
    source_slot = jnp.concatenate([near_slot, far_slot], axis=1)
    pairs = jnp.take(inverse, source_slot, axis=0).astype(jnp.int32)
    return (home, pairs)


def draw_home(key, part):
    return layout_tables(key)[0]


def draw_pairs(key, part):
    return layout_tables(key)[1]


def draw_area(key, part):
    ramp = jnp.arange(BLOCKS, dtype=jnp.float32)[:, None] / (BLOCKS - 1)
    logs = jax.random.uniform(key, (BLOCKS, VERT), jnp.float32, jnp.log(0.2), jnp.log(2.0))
    return jnp.exp(logs) * (0.5 + ramp)


def shard_levels(own_key, extent, cuts, least, largest):
    gain, own = 1.0, jax.random.fold_in(own_key, 6)
    for position, blocks in cuts:
        draws = jnp.exp(jax.random.uniform(jax.random.fold_in(own, position), (blocks,), jnp.float32, least / len(cuts), largest / len(cuts)))
        gain = gain * jnp.repeat(draws, extent[position] // blocks).reshape([-1 if axis == position else 1 for axis in range(len(extent))])
    return gain


def bell_draw(stream_key, extent, spread, bound, cuts=(), kind=jnp.bfloat16):
    values = spread * jax.random.normal(stream_key, extent, jnp.float32)
    if cuts:
        values = values * shard_levels(stream_key, extent, cuts, -0.22, 0.18)
    return jnp.clip(values, -bound, bound).astype(kind)


def setup_inputs(seed: int = 0) -> dict:
    key_list = jax.random.split(jax.random.key(seed), 8)
    return {
        "transfer": bell_draw(key_list[0], (BLOCKS, CH, VERT), 1.0, 6.0, ((0, 32),)),
        "positions": bell_draw(key_list[1], (BLOCKS, 3, VERT), 1.0, 4.0, ((0, 32),), jnp.float32),
        "normals": bell_draw(key_list[2], (BLOCKS, 3, VERT), 1.0, 4.0, ((0, 32),), jnp.float32),
        "area": draw_area(jax.random.fold_in(key_list[7], 71), 0),
        "albedo": jnp.clip(0.3 + 0.59999996 * jax.random.uniform(key_list[4], (BLOCKS, COLORS, VERT), jnp.float32) ** shard_levels(key_list[4], (BLOCKS, COLORS, VERT), ((0, 32),), -0.2, 0.2), 0.3, 0.9),
        "pairs": draw_pairs(jax.random.fold_in(key_list[7], 71), 0),
        "home": draw_home(jax.random.fold_in(key_list[7], 71), 0),
    }


batch_blocks = 4


def form_tiles(recv_pos, recv_nrm, src_pos, src_nrm, src_area):
    distance = None
    along_p = None
    along_q = None
    for axis_id in range(3):
        gap_vec = src_pos[:, :, axis_id, None, :] - recv_pos[:, None, axis_id, :, None]
        near_term = recv_nrm[:, None, axis_id, :, None] * gap_vec
        far_term = src_nrm[:, :, axis_id, None, :] * gap_vec
        if distance is None:
            distance = gap_vec * gap_vec
            along_p = near_term
            along_q = far_term
        else:
            distance = distance + gap_vec * gap_vec
            along_p = along_p + near_term
            along_q = along_q + far_term
    soft_sq = distance + 1.0
    transfer_factors = jnp.maximum(along_p, 0.0) * jnp.maximum(-along_q, 0.0) * src_area[:, :, None, :] / (jnp.pi * soft_sq * soft_sq)
    return transfer_factors.astype(jnp.bfloat16)


def reflect_all(source_rows, src_positions, src_normals, src_area, pair_row_list, recv_positions, recv_normals):
    turns = pair_row_list.shape[0] // batch_blocks

    def group_term(group_id):
        first_row = group_id * batch_blocks
        picked_rows = lax.dynamic_slice_in_dim(pair_row_list, first_row, batch_blocks, 0)
        recv_pos = lax.dynamic_slice_in_dim(recv_positions, first_row, batch_blocks, 0)
        recv_nrm = lax.dynamic_slice_in_dim(recv_normals, first_row, batch_blocks, 0)
        transfer_factors = form_tiles(recv_pos, recv_nrm, jnp.take(src_positions, picked_rows, axis=0),
                             jnp.take(src_normals, picked_rows, axis=0), jnp.take(src_area, picked_rows, axis=0))
        collected_values = jnp.take(source_rows, picked_rows, axis=0)
        return jnp.einsum('wxmy,wxsy->wms', collected_values.astype(jnp.float32), transfer_factors.astype(jnp.float32))

    summed = lax.map(group_term, jnp.arange(turns, dtype=jnp.int32))
    return summed.reshape((pair_row_list.shape[0],) + source_rows.shape[1:])


def apply_albedo(summed, albedo):
    blocks_here, channels, verts = summed.shape
    shaped = summed.reshape(blocks_here, COLORS, channels // COLORS, verts) * albedo[:, :, None, :]
    return shaped.reshape(blocks_here, channels, verts)


def reference(transfer, positions, normals, area, albedo, pairs, home):
    slot_ids = jnp.take(home, pairs, axis=0)
    first_bounce = apply_albedo(reflect_all(transfer, positions, normals, area, slot_ids, positions, normals), albedo)
    bounce_one = first_bounce.astype(jnp.bfloat16)
    second_bounce = apply_albedo(reflect_all(bounce_one, positions, normals, area, slot_ids, positions, normals), albedo)
    bounce_two = second_bounce.astype(jnp.bfloat16)
    inv_count = 1.0 / (BLOCKS * VERT * CH)
    energy_one = jnp.sum(area[:, None, :] * first_bounce * first_bounce) * inv_count
    energy_two = jnp.sum(area[:, None, :] * second_bounce * second_bounce) * inv_count
    energies = jnp.stack([energy_one, energy_two]).astype(jnp.float32)
    return bounce_one, bounce_two, energies
```

```python
import functools

import jax
import jax.numpy as jnp
from jax import lax
from jax.experimental import pallas as pl
from jax.experimental.pallas import tpu as pltpu
from jax.sharding import PartitionSpec as P

COLORS = 3
NEAR = 16
CAP = 2
AXES = ("gx", "gy")
VMEM_LIMIT = 62 * 1024 * 1024
MESH = pl.DeviceIdType.MESH


def split3(f):
    hi = f.astype(jnp.bfloat16).astype(jnp.float32)
    rest = f - hi
    mid = rest.astype(jnp.bfloat16).astype(jnp.float32)
    return hi, mid, rest - mid


def source_features(pos, m):
    lanes = pos.shape[1]
    sq = jnp.sum(pos * pos, axis=0, keepdims=True)
    d = -jnp.sum(m * pos, axis=0, keepdims=True)
    hi, mid, lo = split3(jnp.concatenate([pos, sq, m, d], axis=0))
    ones = jnp.ones((8, lanes), jnp.float32)
    half = jnp.concatenate([hi, hi, hi, mid, mid, lo, ones, jnp.zeros_like(ones)], axis=0)
    return jnp.concatenate([half, half], axis=0).T


def receiver_weights(pos, nrm):
    lanes = pos.shape[1]
    zero3 = jnp.zeros((3, lanes), jnp.float32)
    zero1 = jnp.zeros((1, lanes), jnp.float32)
    one1 = jnp.ones((1, lanes), jnp.float32)
    zero5 = jnp.zeros((5, lanes), jnp.float32)
    zero8 = jnp.zeros((8, lanes), jnp.float32)

    def column(feat, const):
        hi, mid, lo = split3(feat)
        chi, cmid, clo = split3(const)
        return jnp.concatenate(
            [hi, mid, lo, hi, mid, hi, jnp.concatenate([chi, cmid, clo, zero5], axis=0), zero8],
            axis=0,
        )

    dist = column(
        jnp.concatenate([-2.0 * pos, one1, zero3, zero1], axis=0),
        jnp.sum(pos * pos, axis=0, keepdims=True) + 1.0,
    )
    along_p = column(
        jnp.concatenate([nrm, zero1, zero3, zero1], axis=0),
        -jnp.sum(nrm * pos, axis=0, keepdims=True),
    )
    along_q = column(jnp.concatenate([zero3, zero1, pos, one1], axis=0), zero1)
    return jnp.concatenate([dist, along_p, along_q], axis=1)


def block_diag(w):
    z = jnp.zeros_like(w)
    return jnp.concatenate(
        [jnp.concatenate([w, z], axis=1), jnp.concatenate([z, w], axis=1)], axis=0
    ).astype(jnp.bfloat16)


def row_tiles(rows_ref, slot, base, weights, feats, tiles):
    v = tiles.shape[-1]
    first = lax.broadcasted_iota(jnp.int32, (v, v), 1) < v // 2
    for i in range(rows_ref.shape[1] // 4):
        t = [rows_ref[slot, i * 4 + j] for j in range(4)]
        x = jnp.concatenate(
            [
                jnp.where(first, feats[t[0]], feats[t[1]]),
                jnp.where(first, feats[t[2]], feats[t[3]]),
            ],
            axis=0,
        )
        g = jnp.dot(x, weights, preferred_element_type=jnp.float32)
        for j in range(4):
            r, c = (j // 2) * v, (j % 2) * 3 * v
            dist = g[r : r + v, c : c + v]
            ap = g[r : r + v, c + v : c + 2 * v]
            aq = g[r : r + v, c + 2 * v : c + 3 * v]
            f = jnp.maximum(ap, 0.0) * jnp.maximum(aq, 0.0) / (dist * dist)
            at = base + (i * 4 + j) * v
            tiles[slot, at : at + v, :] = f.astype(jnp.bfloat16)


def contract(rows_ref, slot, base, field, tiles):
    v = tiles.shape[-1]
    count = rows_ref.shape[1]
    picked = jnp.concatenate([field[rows_ref[slot, j]] for j in range(count)], axis=1)
    return jnp.dot(
        picked, tiles[slot, base : base + count * v, :], preferred_element_type=jnp.float32
    )


def bounce_kernel(
    n, ny, ch, cuts,
    pairs, home, transfer, positions, normals, area, albedo,
    one_hbm, two_hbm, energy_ref,
    *scratch,
):
    (
        near_rows, far_ids, far_rows, low_s, req_s,
        tr, raw_pos, raw_nrm, raw_area, raw_alb, geo, wire, field,
        geo_out, geo_in, near_feats, far_feats, wts, tiles,
        req_v, req_in, acc, one, two, out1, out2, en, en_in,
    ) = scratch[:28]
    k = len(cuts)
    box_out = scratch[28 : 28 + k]
    box_in = scratch[28 + k : 28 + 2 * k]
    box_in2 = scratch[28 + 2 * k : 28 + 3 * k]
    sems = scratch[28 + 3 * k :]
    loc, pair_sems = sems[0], sems[1:]
    bf16, f32, i32 = jnp.bfloat16, jnp.float32, jnp.int32

    gx, gy = lax.axis_index("gx"), lax.axis_index("gy")
    me = gx * ny + gy
    b, v = area.shape
    near = near_rows.shape[1]
    far = far_ids.shape[1]

    def peer(d):
        t = lax.rem(me + d, n)
        return t, (lax.div(t, ny), lax.rem(t, ny))

    def each_peer(fn):
        def step(d, carry):
            fn(d)
            return carry

        lax.fori_loop(1, n, step, 0)

    def copies(which, src, dst):
        send, recv = pair_sems[2 * which], pair_sems[2 * which + 1]

        def make(d):
            t, dev = peer(d)
            return pltpu.make_async_remote_copy(
                src_ref=src(t), dst_ref=dst, send_sem=send.at[d], recv_sem=recv.at[d],
                device_id=dev, device_id_type=MESH,
            )

        return make

    def pair(ref, t):
        return ref.at[pl.ds(t * CAP, CAP)]

    req_cp = copies(0, lambda t: req_v.at[0], req_in.at[me])
    geo_cp = copies(1, lambda t: geo_out.at[t], geo_in.at[me])
    en_cp = copies(2, lambda t: en, en_in.at[me])

    def field_cp(i, which, box):
        return copies(which, lambda t: pair(box_out[i], t), pair(box[i], me))

    first_cp = [field_cp(i, 3 + i, box_in) for i in range(k)]
    second_cp = [field_cp(i, 3 + k + i, box_in2) for i in range(k)]

    barrier = pltpu.get_barrier_semaphore()
    each_peer(lambda d: pl.semaphore_signal(barrier, inc=1, device_id=peer(d)[1], device_id_type=MESH))
    loads = [
        pltpu.make_async_copy(src, dst, loc.at[i])
        for i, (src, dst) in enumerate(
            [
                (positions, raw_pos), (normals, raw_nrm), (area, raw_area),
                (albedo, raw_alb), (transfer, tr),
            ]
        )
    ]
    for cp in loads:
        cp.start()

    lanes = req_v.shape[2]
    floor = lax.broadcasted_iota(i32, (1, lanes), 1) * b

    def scan(s, carry):
        low, high = carry
        for j in range(near):
            near_rows[s, j] = lax.rem(home[pairs[s, j]], b)
        for j in range(far):
            t = home[pairs[s, near + j]]
            far_ids[s, j] = t
            x = t - floor
            ok = (x >= 0) & (x < b)
            low = jnp.minimum(low, jnp.where(ok, x, b - 1))
            high = jnp.maximum(high, jnp.where(ok, x, 0))
        return low, high

    low, high = lax.fori_loop(
        0, b, scan, (jnp.full((1, lanes), b - 1, i32), jnp.zeros((1, lanes), i32))
    )
    req_v[0] = low + high * b
    req_v[1] = low
    req_in[me] = jnp.zeros((1, lanes), i32)
    low_cp = pltpu.make_async_copy(req_v.at[1], low_s, loc.at[5])
    low_cp.start()

    for cp in loads[:4]:
        cp.wait()
    m = raw_nrm[...] * (raw_area[...] * (1.0 / jnp.pi))[None]
    p_hi, p_mid, _ = split3(raw_pos[...])
    m_hi, m_mid, _ = split3(m)
    geo[...] = jnp.swapaxes(
        jnp.concatenate(
            [raw_pos[...], m, raw_nrm[...], raw_area[...][None], raw_alb[...],
             jnp.zeros((3, b, v), f32)], axis=0
        ),
        0, 1,
    )
    wire[...] = jnp.swapaxes(
        jnp.concatenate([p_hi, p_mid, m_hi, m_mid, jnp.zeros((4, b, v), f32)], axis=0), 0, 1
    ).astype(bf16)
    loads[4].wait()
    for lo, hi in cuts:
        part = tr[lo : min(hi, ch)]
        if hi > ch:
            part = jnp.concatenate([part, jnp.zeros((hi - ch, b, v), bf16)], axis=0)
        field[:, lo:hi] = jnp.swapaxes(part, 0, 1)

    def table(read, count, feats):
        def step(t, carry):
            for i in range(4):
                feats[t * 4 + i] = source_features(*read(t * 4 + i)).astype(bf16)
            return carry

        lax.fori_loop(0, count // 4, step, 0)

    table(lambda t: (geo[t, 0:3], geo[t, 3:6]), b, near_feats)

    def near_slots(lo, hi):
        def step(s, carry):
            w = block_diag(receiver_weights(geo[s, 0:3], geo[s, 6:9]))
            wts[s] = w
            row_tiles(near_rows, s, 0, w, near_feats, tiles)
            return carry

        lax.fori_loop(lo, hi, step, 0, unroll=2)

    pl.semaphore_wait(barrier, n - 1)
    each_peer(lambda d: req_cp(d).start())
    near_slots(0, b // 4)
    for box in (geo_in,) + tuple(box_in) + tuple(box_in2):
        each = box.shape[0] // n
        for c in range(each):
            box[me * each + c] = jnp.zeros(box.shape[1:], box.dtype)
    each_peer(lambda d: req_cp(d).wait())
    ask_cp = pltpu.make_async_copy(req_in, req_s, loc.at[0])
    ask_cp.start()
    ask_cp.wait()

    def pack(put):
        def step(t, carry):
            r = req_s[t, 0, me]
            hi = lax.div(r, b)
            put(t, r - hi * b, hi)
            return carry

        lax.fori_loop(0, n, step, 0)

    def put_geo(t, x, y):
        geo_out[t] = jnp.concatenate([wire[x, 0:12], wire[y, 0:12]], axis=0)

    def put_field(i, source):
        lo, hi = cuts[i]

        def put(t, x, y):
            box_out[i][t * CAP] = source[x, lo:hi]
            box_out[i][t * CAP + 1] = source[y, lo:hi]

        return put

    pack(put_geo)
    each_peer(lambda d: geo_cp(d).start())
    for i in range(k):
        pack(put_field(i, field))
        each_peer(lambda d: first_cp[i](d).start())

    low_cp.wait()

    def far_index(s, carry):
        for j in range(far):
            t = far_ids[s, j]
            owner = lax.div(t, b)
            far_rows[s, j] = owner * CAP + (t - owner * b > low_s[0, owner]).astype(i32)
        return carry

    lax.fori_loop(0, b, far_index, 0)
    near_slots(b // 4, b)
    each_peer(lambda d: geo_cp(d).wait())

    def far_geo(t):
        g = geo_in[t].astype(f32)
        return [(g[q : q + 3] + g[q + 3 : q + 6], g[q + 6 : q + 9] + g[q + 9 : q + 12]) for q in (0, 12)]

    def far_table(t, carry):
        for i in range(2):
            for c, g in enumerate(far_geo(t * 2 + i)):
                far_feats[(t * 2 + i) * CAP + c] = source_features(*g).astype(bf16)
        return carry

    lax.fori_loop(0, n // 2, far_table, 0)

    def far_slot(s, carry):
        row_tiles(far_rows, s, near * v, wts[s], far_feats, tiles)
        return carry

    lax.fori_loop(0, b, far_slot, 0, unroll=2)

    def near_sum(source):
        def step(s, carry):
            acc[s] = contract(near_rows, s, 0, source, tiles)
            return carry

        lax.fori_loop(0, b, step, 0, unroll=2)

    near_sum(field)

    def finish(i, box, write):
        lo, hi = cuts[i]
        row = lax.broadcasted_iota(i32, (hi - lo, v), 0) + lo

        def step(s, e):
            total = acc[s, lo:hi] + contract(far_rows, s, near * v, box[i], tiles)
            shade = jnp.broadcast_to(geo[s, 12:13, :], (hi - lo, v))
            for c in range(COLORS - 2, -1, -1):
                shade = jnp.where(row < (c + 1) * (ch // COLORS), geo[s, 10 + c : 11 + c, :], shade)
            val = total * shade
            keep = val if hi <= ch else jnp.where(row < ch, val, 0.0)
            write(s, lo, hi, val.astype(bf16))
            return e + jnp.sum(keep * keep, axis=0, keepdims=True) * geo[s, 9:10, :]

        return lambda e: lax.fori_loop(0, b, step, e, unroll=2)

    def planes(source, out, i):
        lo, hi = cuts[i]
        top = min(hi, ch)
        out[lo:top] = jnp.swapaxes(source[:, lo:hi], 0, 1)[0 : top - lo]

    def keep(ref):
        def write(s, lo, hi, val):
            ref[s, lo:hi] = val

        return write

    e1 = jnp.zeros((1, v), f32)
    for i in range(k):
        each_peer(lambda d: first_cp[i](d).wait())
        e1 = finish(i, box_in, keep(one))(e1)
        pack(put_field(i, one))
        each_peer(lambda d: second_cp[i](d).start())
        planes(one, out1, i)
    one_cp = pltpu.make_async_copy(out1, one_hbm, loc.at[0])
    one_cp.start()
    near_sum(one)
    e2 = jnp.zeros((1, v), f32)
    for i in range(k):
        each_peer(lambda d: second_cp[i](d).wait())
        e2 = finish(i, box_in2, keep(two))(e2)
        if i < k - 1:
            planes(two, out2, i)
    en[...] = jnp.concatenate([e1, e2], axis=0)
    en_in[me] = en[...]
    each_peer(lambda d: en_cp(d).start())
    planes(two, out2, k - 1)
    two_cp = pltpu.make_async_copy(out2, two_hbm, loc.at[1])
    two_cp.start()
    one_cp.wait()
    each_peer(lambda d: en_cp(d).wait())
    total = jnp.sum(en_in[...], axis=0) * (1.0 / (n * b * v * ch))
    energy_ref[0] = jnp.sum(total[0:1])
    energy_ref[1] = jnp.sum(total[1:2])
    two_cp.wait()


def body(transfer, positions, normals, area, albedo, pairs, home):
    n = lax.axis_size(AXES)
    b, ch, v = transfer.shape
    far = pairs.shape[1] - NEAR
    rows = -(-ch // 16) * 16
    cut = -(-rows // 32) * 16
    cuts = ((0, cut), (cut, rows))
    bf16, f32, i32 = jnp.bfloat16, jnp.float32, jnp.int32
    lanes = -(-n // 128) * 128

    smem = pl.BlockSpec(memory_space=pltpu.SMEM)
    hbm = pl.BlockSpec(memory_space=pl.ANY)
    sem = pltpu.SemaphoreType.DMA((n,))
    boxes = [pltpu.VMEM((n * CAP, hi - lo, v), bf16) for lo, hi in cuts]
    one, two, energies = pl.pallas_call(
        functools.partial(bounce_kernel, n, lax.axis_size("gy"), ch, cuts),
        name="bounces",
        in_specs=[smem, smem] + [hbm] * 5,
        out_specs=[hbm, hbm, smem],
        out_shape=[
            jax.ShapeDtypeStruct((ch, b, v), bf16),
            jax.ShapeDtypeStruct((ch, b, v), bf16),
            jax.ShapeDtypeStruct((2,), f32),
        ],
        scratch_shapes=[
            pltpu.SMEM((b, NEAR), i32),
            pltpu.SMEM((b, far), i32),
            pltpu.SMEM((b, far), i32),
            pltpu.SMEM((1, lanes), i32),
            pltpu.SMEM((n, 1, lanes), i32),
            pltpu.VMEM((ch, b, v), bf16),
            pltpu.VMEM((3, b, v), f32),
            pltpu.VMEM((3, b, v), f32),
            pltpu.VMEM((b, v), f32),
            pltpu.VMEM((3, b, v), f32),
            pltpu.VMEM((b, 16, v), f32),
            pltpu.VMEM((b, 16, v), bf16),
            pltpu.VMEM((b, rows, v), bf16),
            pltpu.VMEM((n, 24, v), bf16),
            pltpu.VMEM((n, 24, v), bf16),
            pltpu.VMEM((b, v, v), bf16),
            pltpu.VMEM((n * CAP, v, v), bf16),
            pltpu.VMEM((b, v, 6 * v), bf16),
            pltpu.VMEM((b, (NEAR + far) * v, v), bf16),
            pltpu.VMEM((2, 1, lanes), i32),
            pltpu.VMEM((n, 1, lanes), i32),
            pltpu.VMEM((b, rows, v), f32),
            pltpu.VMEM((b, rows, v), bf16),
            pltpu.VMEM((b, rows, v), bf16),
            pltpu.VMEM((ch, b, v), bf16),
            pltpu.VMEM((ch, b, v), bf16),
            pltpu.VMEM((2, v), f32),
            pltpu.VMEM((n, 2, v), f32),
        ]
        + boxes * 3
        + [pltpu.SemaphoreType.DMA((6,))]
        + [sem] * (6 + 4 * len(cuts)),
        compiler_params=pltpu.CompilerParams(
            collective_id=0, has_side_effects=True, vmem_limit_bytes=VMEM_LIMIT
        ),
    )(
        pairs, home,
        jnp.swapaxes(transfer, 0, 1), jnp.swapaxes(positions, 0, 1),
        jnp.swapaxes(normals, 0, 1), area, jnp.swapaxes(albedo, 0, 1),
    )
    return jnp.swapaxes(one, 0, 1), jnp.swapaxes(two, 0, 1), energies


def solution(mesh):
    return jax.shard_map(
        body,
        mesh=mesh,
        in_specs=(
            P(AXES, None, None),
            P(AXES, None, None),
            P(AXES, None, None),
            P(AXES, None),
            P(AXES, None, None),
            P(AXES, None),
            P(),
        ),
        out_specs=(P(AXES, None, None), P(AXES, None, None), P()),
        check_vma=False,
    )
```

```python
import functools

import jax
import jax.numpy as jnp
from jax import lax
from jax.experimental import pallas as pl
from jax.experimental.pallas import tpu as pltpu
from jax.sharding import PartitionSpec as P

COLORS = 3
NEAR = 16
CAP = 2
AXES = ("gx", "gy")
VMEM_LIMIT = 62 * 1024 * 1024
MESH = pl.DeviceIdType.MESH


def split3(f):
    hi = f.astype(jnp.bfloat16).astype(jnp.float32)
    rest = f - hi
    mid = rest.astype(jnp.bfloat16).astype(jnp.float32)
    return hi, mid, rest - mid


def source_features(pos, m):
    lanes = pos.shape[1]
    sq = jnp.sum(pos * pos, axis=0, keepdims=True)
    d = -jnp.sum(m * pos, axis=0, keepdims=True)
    hi, mid, lo = split3(jnp.concatenate([pos, sq, m, d], axis=0))
    ones = jnp.ones((8, lanes), jnp.float32)
    half = jnp.concatenate([hi, hi, hi, mid, mid, lo, ones, jnp.zeros_like(ones)], axis=0)
    return jnp.concatenate([half, half], axis=0).T


def receiver_weights(pos, nrm):
    lanes = pos.shape[1]
    zero3 = jnp.zeros((3, lanes), jnp.float32)
    zero1 = jnp.zeros((1, lanes), jnp.float32)
    one1 = jnp.ones((1, lanes), jnp.float32)
    zero5 = jnp.zeros((5, lanes), jnp.float32)
    zero8 = jnp.zeros((8, lanes), jnp.float32)

    def column(feat, const):
        hi, mid, lo = split3(feat)
        chi, cmid, clo = split3(const)
        return jnp.concatenate(
            [hi, mid, lo, hi, mid, hi, jnp.concatenate([chi, cmid, clo, zero5], axis=0), zero8],
            axis=0,
        )

    dist = column(
        jnp.concatenate([-2.0 * pos, one1, zero3, zero1], axis=0),
        jnp.sum(pos * pos, axis=0, keepdims=True) + 1.0,
    )
    along_p = column(
        jnp.concatenate([nrm, zero1, zero3, zero1], axis=0),
        -jnp.sum(nrm * pos, axis=0, keepdims=True),
    )
    along_q = column(jnp.concatenate([zero3, zero1, pos, one1], axis=0), zero1)
    return jnp.concatenate([dist, along_p, along_q], axis=1)


def block_diag(w):
    z = jnp.zeros_like(w)
    return jnp.concatenate(
        [jnp.concatenate([w, z], axis=1), jnp.concatenate([z, w], axis=1)], axis=0
    ).astype(jnp.bfloat16)


def row_tiles(rows_ref, slot, base, weights, feats, tiles, side):
    v = tiles.shape[-1] // 2
    first = lax.broadcasted_iota(jnp.int32, (v, v), 1) < v // 2
    for i in range(rows_ref.shape[1] // 4):
        t = [rows_ref[slot, i * 4 + j] for j in range(4)]
        x = jnp.concatenate(
            [
                jnp.where(first, feats[t[0]], feats[t[1]]),
                jnp.where(first, feats[t[2]], feats[t[3]]),
            ],
            axis=0,
        )
        g = jnp.dot(x, weights, preferred_element_type=jnp.float32)
        for j in range(4):
            r, c = (j // 2) * v, (j % 2) * 3 * v
            dist = g[r : r + v, c : c + v]
            ap = g[r : r + v, c + v : c + 2 * v]
            aq = g[r : r + v, c + 2 * v : c + 3 * v]
            f = jnp.maximum(ap, 0.0) * jnp.maximum(aq, 0.0) / (dist * dist)
            at = base + (i * 4 + j) * v
            tiles[at : at + v, side * v : (side + 1) * v] = f.astype(jnp.bfloat16)


def contract(rows_ref, i, base, field, tiles):
    v = tiles.shape[-1] // 2
    count = rows_ref.shape[1]
    picked = jnp.concatenate(
        [
            jnp.concatenate([field[rows_ref[2 * i + side, j]] for j in range(count)], axis=1)
            for side in range(2)
        ],
        axis=0,
    )
    both = jnp.dot(
        picked, tiles[i, base : base + count * v, :], preferred_element_type=jnp.float32
    )
    rows = both.shape[0] // 2
    return both[0:rows, 0:v], both[rows:, v:]


def bounce_kernel(
    n, ny, ch, cuts,
    pairs, home, transfer, positions, normals, area, albedo,
    one_hbm, two_hbm, energy_ref,
    *scratch,
):
    (
        near_rows, far_ids, far_rows, low_s, req_s,
        tr, raw_pos, raw_nrm, raw_area, raw_alb, geo,
        wire_planes, guest_planes, wire, guest_wire, field,
        geo_own, geo_fwd, geo_in, near_feats, far_feats, wts, tiles,
        req_v, req_in, acc, one, two, out1, out2, en, en_in,
    ) = scratch[:32]
    k = len(cuts)
    groups = [scratch[32 + i * k : 32 + (i + 1) * k] for i in range(7)]
    box_own, box_fwd, box_in, box_in2, guest, planes_in, planes_in2 = groups
    loc, stat_s, stat_r, req_sems, en_sems = scratch[32 + 7 * k : 37 + 7 * k]
    peer_sems = scratch[37 + 7 * k :]
    bf16, f32, i32 = jnp.bfloat16, jnp.float32, jnp.int32

    gx, gy = lax.axis_index("gx"), lax.axis_index("gy")
    me = gx * ny + gy
    h, nh = ny // 2, n // 2
    side = lax.div(gy, h)
    mate_y = lax.rem(gy + h, ny)
    mate = gx * ny + mate_y
    spot = gx * h + gy - side * h
    b, v = area.shape
    near = near_rows.shape[1]
    far = far_ids.shape[1]

    def peer(d):
        t = lax.rem(me + d, n)
        return (lax.div(t, ny), lax.rem(t, ny))

    def side_peer(d):
        t = lax.rem(spot + d, nh)
        return t, (lax.div(t, h), side * h + lax.rem(t, h))

    def each(count, fn):
        def step(d, carry):
            fn(d)
            return carry

        lax.fori_loop(1, count, step, 0)

    def pair(ref, t):
        return ref.at[pl.ds(t * CAP, CAP)]

    class Spread:
        def __init__(self, sems, src, dst):
            self.sems, self.src, self.dst = sems, src, dst

        def copy(self, d):
            t, dev = side_peer(d)
            return pltpu.make_async_remote_copy(
                src_ref=self.src(t), dst_ref=self.dst,
                send_sem=self.sems.at[0, d], recv_sem=self.sems.at[1, d],
                device_id=dev, device_id_type=MESH,
            )

        def start(self):
            each(nh, lambda d: self.copy(d).start())

        def wait(self):
            each(nh, lambda d: self.copy(d).wait())

    def to_mate(i, src, dst):
        return pltpu.make_async_remote_copy(
            src_ref=src, dst_ref=dst, send_sem=stat_s.at[i], recv_sem=stat_r.at[i],
            device_id=(gx, mate_y), device_id_type=MESH,
        )

    def en_copy(d):
        return pltpu.make_async_remote_copy(
            src_ref=en, dst_ref=en_in.at[me],
            send_sem=en_sems.at[0, d], recv_sem=en_sems.at[1, d],
            device_id=peer(d), device_id_type=MESH,
        )

    req_x = Spread(req_sems, lambda t: req_v.at[0], req_in.at[spot])
    geo_x = [
        Spread(peer_sems[0], lambda t: geo_own.at[t], geo_in.at[me]),
        Spread(peer_sems[1], lambda t: geo_fwd.at[t], geo_in.at[mate]),
    ]

    def field_x(i, base, box):
        return [
            Spread(peer_sems[base], lambda t: pair(box_own[i], t), pair(box[i], me)),
            Spread(peer_sems[base + 1], lambda t: pair(box_fwd[i], t), pair(box[i], mate)),
        ]

    first_x = [field_x(i, 2 + 2 * i, box_in) for i in range(k)]
    second_x = [field_x(i, 2 + 2 * k + 2 * i, box_in2) for i in range(k)]
    tops = [min(hi, ch) for lo, hi in cuts]
    geo_m = to_mate(0, wire_planes, guest_planes)
    first_m = [
        to_mate(1 + i, tr.at[pl.ds(lo, tops[i] - lo)], planes_in[i])
        for i, (lo, hi) in enumerate(cuts)
    ]
    second_m = [
        to_mate(1 + k + i, out1.at[pl.ds(lo, tops[i] - lo)], planes_in2[i])
        for i, (lo, hi) in enumerate(cuts)
    ]

    barrier = pltpu.get_barrier_semaphore()
    each(n, lambda d: pl.semaphore_signal(barrier, inc=1, device_id=peer(d), device_id_type=MESH))
    loads = [
        pltpu.make_async_copy(src, dst, loc.at[i])
        for i, (src, dst) in enumerate(
            [
                (positions, raw_pos), (normals, raw_nrm), (area, raw_area),
                (albedo, raw_alb), (transfer, tr),
            ]
        )
    ]
    for cp in loads:
        cp.start()

    lanes = req_v.shape[2]
    floor = lax.broadcasted_iota(i32, (1, lanes), 1) * b

    def scan(s, carry):
        low, high = carry
        for j in range(near):
            near_rows[s, j] = lax.rem(home[pairs[s, j]], b)
        for j in range(far):
            t = home[pairs[s, near + j]]
            far_ids[s, j] = t
            x = t - floor
            ok = (x >= 0) & (x < b)
            low = jnp.minimum(low, jnp.where(ok, x, b - 1))
            high = jnp.maximum(high, jnp.where(ok, x, 0))
        return low, high

    low, high = lax.fori_loop(
        0, b, scan, (jnp.full((1, lanes), b - 1, i32), jnp.zeros((1, lanes), i32))
    )
    req_v[0] = low + high * b
    req_v[1] = low
    req_in[spot] = low + high * b
    low_cp = pltpu.make_async_copy(req_v.at[1], low_s, loc.at[5])
    low_cp.start()

    for cp in loads[:4]:
        cp.wait()
    m = raw_nrm[...] * (raw_area[...] * (1.0 / jnp.pi))[None]
    p_hi, p_mid, _ = split3(raw_pos[...])
    m_hi, m_mid, _ = split3(m)
    geo[...] = jnp.swapaxes(
        jnp.concatenate(
            [raw_pos[...], m, raw_nrm[...], raw_area[...][None], raw_alb[...],
             jnp.zeros((3, b, v), f32)], axis=0
        ),
        0, 1,
    )
    planes = jnp.concatenate([p_hi, p_mid, m_hi, m_mid], axis=0)
    wire_planes[...] = planes.astype(bf16)
    wire[...] = jnp.swapaxes(
        jnp.concatenate([planes, jnp.zeros((4, b, v), f32)], axis=0), 0, 1
    ).astype(bf16)
    loads[4].wait()

    def rows_of(source, i, base):
        lo, hi = cuts[i]
        part = source[lo - base : tops[i] - base]
        if hi > ch:
            part = jnp.concatenate([part, jnp.zeros((hi - ch, b, v), bf16)], axis=0)
        return jnp.swapaxes(part, 0, 1)

    for i, (lo, hi) in enumerate(cuts):
        field[:, lo:hi] = rows_of(tr, i, 0)

    def table(read, count, feats):
        def step(t, carry):
            for i in range(4):
                feats[t * 4 + i] = source_features(*read(t * 4 + i)).astype(bf16)
            return carry

        lax.fori_loop(0, count // 4, step, 0)

    table(lambda t: (geo[t, 0:3], geo[t, 3:6]), b, near_feats)

    def near_slots(lo, hi):
        def step(i, carry):
            for side in range(2):
                s = 2 * i + side
                w = block_diag(receiver_weights(geo[s, 0:3], geo[s, 6:9]))
                wts[s] = w
                row_tiles(near_rows, s, 0, w, near_feats, tiles.at[i], side)
            return carry

        lax.fori_loop(lo // 2, hi // 2, step, 0)

    pl.semaphore_wait(barrier, n - 1)
    req_x.start()
    for cp in [geo_m] + first_m[:1]:
        cp.start()
    near_slots(0, b // 4)
    for box in (geo_in,) + tuple(box_in) + tuple(box_in2):
        width = box.shape[0] // n
        for c in range(width):
            box[me * width + c] = jnp.zeros(box.shape[1:], box.dtype)
    req_x.wait()
    ask_cp = pltpu.make_async_copy(req_in, req_s, loc.at[0])
    ask_cp.start()
    ask_cp.wait()

    def asked(t, dev):
        r = req_s[t, 0, dev]
        hi = lax.div(r, b)
        return r - hi * b, hi

    def pack(dev, put):
        def step(t, carry):
            put(t, *asked(t, dev))
            return carry

        lax.fori_loop(0, nh, step, 0)

    def geo_pair(source, x, y):
        return jnp.concatenate([source[x, 0:12], source[y, 0:12]], axis=0)

    def send_geo(x, dev, source, out):
        def put(t, p, q):
            out[t] = geo_pair(source, p, q)

        pack(dev, put)
        x.start()

    def send_field(x, dev, read, out):
        def put(t, p, q):
            out[t * CAP] = read(p)
            out[t * CAP + 1] = read(q)

        pack(dev, put)
        x.start()

    def send_own(i, x, source):
        lo, hi = cuts[i]
        send_field(x[0], me, lambda t: source[t, lo:hi], box_own[i])

    def send_guest(i, x, m, source, box):
        m.wait()
        guest[i][...] = rows_of(source[i], i, cuts[i][0])
        send_field(x[1], mate, lambda t: guest[i][t], box_fwd[i])
        for c, t in enumerate(asked(spot, mate)):
            box[i][mate * CAP + c] = guest[i][t]

    send_geo(geo_x[0], me, wire, geo_own)
    geo_m.wait()
    guest_wire[...] = jnp.swapaxes(
        jnp.concatenate([guest_planes[...].astype(f32), jnp.zeros((4, b, v), f32)], axis=0), 0, 1
    ).astype(bf16)
    send_geo(geo_x[1], mate, guest_wire, geo_fwd)
    for cp in first_m[1:]:
        cp.start()
    geo_in[mate] = geo_pair(guest_wire, *asked(spot, mate))
    send_own(0, first_x[0], field)

    low_cp.wait()

    def far_index(s, carry):
        for j in range(far):
            t = far_ids[s, j]
            owner = lax.div(t, b)
            far_rows[s, j] = owner * CAP + (t - owner * b > low_s[0, owner]).astype(i32)
        return carry

    lax.fori_loop(0, b, far_index, 0)
    near_slots(b // 4, 3 * b // 4)
    near_slots(3 * b // 4, b)
    def near_sum(source):
        def step(i, carry):
            acc[2 * i], acc[2 * i + 1] = contract(near_rows, i, 0, source, tiles)
            return carry

        lax.fori_loop(0, b // 2, step, 0, unroll=4)

    near_sum(field)
    for x in geo_x:
        x.wait()
    send_guest(0, first_x[0], first_m[0], planes_in, box_in)
    for i in range(1, k):
        send_own(i, first_x[i], field)

    def far_geo(t):
        g = geo_in[t].astype(f32)
        return [(g[q : q + 3] + g[q + 3 : q + 6], g[q + 6 : q + 9] + g[q + 9 : q + 12]) for q in (0, 12)]

    def far_table(t, carry):
        for i in range(4):
            for c, g in enumerate(far_geo(t * 4 + i)):
                far_feats[(t * 4 + i) * CAP + c] = source_features(*g).astype(bf16)
        return carry

    lax.fori_loop(0, n // 4, far_table, 0)

    def far_slot(i, carry):
        for side in range(2):
            s = 2 * i + side
            row_tiles(far_rows, s, near * v, wts[s], far_feats, tiles.at[i], side)
        return carry

    lax.fori_loop(0, b // 8, far_slot, 0)
    for i in range(1, k):
        send_guest(i, first_x[i], first_m[i], planes_in, box_in)
    lax.fori_loop(b // 8, b // 2, far_slot, 0)

    def finish(i, box, write):
        lo, hi = cuts[i]
        row = lax.broadcasted_iota(i32, (hi - lo, v), 0) + lo

        def step(pair_id, e):
            sums = contract(far_rows, pair_id, near * v, box[i], tiles)
            for side in range(2):
                s = 2 * pair_id + side
                total = acc[s, lo:hi] + sums[side]
                shade = jnp.broadcast_to(geo[s, 12:13, :], (hi - lo, v))
                for c in range(COLORS - 2, -1, -1):
                    shade = jnp.where(
                        row < (c + 1) * (ch // COLORS), geo[s, 10 + c : 11 + c, :], shade
                    )
                val = total * shade
                keep = val if hi <= ch else jnp.where(row < ch, val, 0.0)
                write(s, lo, hi, val.astype(bf16))
                e = e + jnp.sum(keep * keep, axis=0, keepdims=True) * geo[s, 9:10, :]
            return e

        return lambda e: lax.fori_loop(0, b // 2, step, e, unroll=4)

    def to_planes(source, out, i):
        lo, hi = cuts[i]
        out[lo : tops[i]] = jnp.swapaxes(source[:, lo:hi], 0, 1)[0 : tops[i] - lo]

    def keep(ref):
        def write(s, lo, hi, val):
            ref[s, lo:hi] = val

        return write

    e1 = jnp.zeros((1, v), f32)
    for i in range(k):
        for x in first_x[i]:
            x.wait()
        e1 = finish(i, box_in, keep(one))(e1)
        to_planes(one, out1, i)
        second_m[i].start()
        send_own(i, second_x[i], one)
    one_cp = pltpu.make_async_copy(out1, one_hbm, loc.at[0])
    one_cp.start()
    send_guest(0, second_x[0], second_m[0], planes_in2, box_in2)
    near_sum(one)
    for i in range(1, k):
        send_guest(i, second_x[i], second_m[i], planes_in2, box_in2)
    e2 = jnp.zeros((1, v), f32)
    for i in range(k):
        for x in second_x[i]:
            x.wait()
        e2 = finish(i, box_in2, keep(two))(e2)
        if i < k - 1:
            to_planes(two, out2, i)
    en[...] = jnp.concatenate([e1, e2], axis=0)
    en_in[me] = en[...]
    each(n, lambda d: en_copy(d).start())
    to_planes(two, out2, k - 1)
    two_cp = pltpu.make_async_copy(out2, two_hbm, loc.at[1])
    two_cp.start()
    one_cp.wait()
    each(n, lambda d: en_copy(d).wait())
    total = jnp.sum(en_in[...], axis=0) * (1.0 / (n * b * v * ch))
    energy_ref[0] = jnp.sum(total[0:1])
    energy_ref[1] = jnp.sum(total[1:2])
    two_cp.wait()


def body(transfer, positions, normals, area, albedo, pairs, home):
    n = lax.axis_size(AXES)
    b, ch, v = transfer.shape
    far = pairs.shape[1] - NEAR
    rows = -(-ch // 16) * 16
    cut = -(-rows // 32) * 16
    cuts = ((0, cut), (cut, rows))
    bf16, f32, i32 = jnp.bfloat16, jnp.float32, jnp.int32
    lanes = -(-n // 128) * 128

    smem = pl.BlockSpec(memory_space=pltpu.SMEM)
    hbm = pl.BlockSpec(memory_space=pl.ANY)
    nh = n // 2
    sem = pltpu.SemaphoreType.DMA((2, nh))
    sizes = [hi - lo for lo, hi in cuts]
    boxes = [pltpu.VMEM((nh * CAP, size, v), bf16) for size in sizes] * 2
    boxes += [pltpu.VMEM((n * CAP, size, v), bf16) for size in sizes] * 2
    boxes += [pltpu.VMEM((b, size, v), bf16) for size in sizes]
    boxes += [pltpu.VMEM((min(hi, ch) - lo, b, v), bf16) for lo, hi in cuts] * 2
    one, two, energies = pl.pallas_call(
        functools.partial(bounce_kernel, n, lax.axis_size("gy"), ch, cuts),
        name="bounces",
        in_specs=[smem, smem] + [hbm] * 5,
        out_specs=[hbm, hbm, smem],
        out_shape=[
            jax.ShapeDtypeStruct((ch, b, v), bf16),
            jax.ShapeDtypeStruct((ch, b, v), bf16),
            jax.ShapeDtypeStruct((2,), f32),
        ],
        scratch_shapes=[
            pltpu.SMEM((b, NEAR), i32),
            pltpu.SMEM((b, far), i32),
            pltpu.SMEM((b, far), i32),
            pltpu.SMEM((1, lanes), i32),
            pltpu.SMEM((nh, 1, lanes), i32),
            pltpu.VMEM((ch, b, v), bf16),
            pltpu.VMEM((3, b, v), f32),
            pltpu.VMEM((3, b, v), f32),
            pltpu.VMEM((b, v), f32),
            pltpu.VMEM((3, b, v), f32),
            pltpu.VMEM((b, 16, v), f32),
            pltpu.VMEM((12, b, v), bf16),
            pltpu.VMEM((12, b, v), bf16),
            pltpu.VMEM((b, 16, v), bf16),
            pltpu.VMEM((b, 16, v), bf16),
            pltpu.VMEM((b, rows, v), bf16),
            pltpu.VMEM((nh, 24, v), bf16),
            pltpu.VMEM((nh, 24, v), bf16),
            pltpu.VMEM((n, 24, v), bf16),
            pltpu.VMEM((b, v, v), bf16),
            pltpu.VMEM((n * CAP, v, v), bf16),
            pltpu.VMEM((b, v, 6 * v), bf16),
            pltpu.VMEM((b // 2, (NEAR + far) * v, 2 * v), bf16),
            pltpu.VMEM((2, 1, lanes), i32),
            pltpu.VMEM((nh, 1, lanes), i32),
            pltpu.VMEM((b, rows, v), f32),
            pltpu.VMEM((b, rows, v), bf16),
            pltpu.VMEM((b, rows, v), bf16),
            pltpu.VMEM((ch, b, v), bf16),
            pltpu.VMEM((ch, b, v), bf16),
            pltpu.VMEM((2, v), f32),
            pltpu.VMEM((n, 2, v), f32),
        ]
        + boxes
        + [pltpu.SemaphoreType.DMA((6,))]
        + [pltpu.SemaphoreType.DMA((1 + 2 * len(cuts),))] * 2
        + [sem, pltpu.SemaphoreType.DMA((2, n))]
        + [sem] * (2 + 4 * len(cuts)),
        compiler_params=pltpu.CompilerParams(
            collective_id=0, has_side_effects=True, vmem_limit_bytes=VMEM_LIMIT
        ),
    )(
        pairs, home,
        jnp.swapaxes(transfer, 0, 1), jnp.swapaxes(positions, 0, 1),
        jnp.swapaxes(normals, 0, 1), area, jnp.swapaxes(albedo, 0, 1),
    )
    return jnp.swapaxes(one, 0, 1), jnp.swapaxes(two, 0, 1), energies


def solution(mesh):
    return jax.shard_map(
        body,
        mesh=mesh,
        in_specs=(
            P(AXES, None, None),
            P(AXES, None, None),
            P(AXES, None, None),
            P(AXES, None),
            P(AXES, None, None),
            P(AXES, None),
            P(),
        ),
        out_specs=(P(AXES, None, None), P(AXES, None, None), P()),
        check_vma=False,
    )
```

```python
import functools

import jax
import jax.numpy as jnp
from jax import lax
from jax.experimental import pallas as pl
from jax.experimental.pallas import tpu as pltpu
from jax.sharding import PartitionSpec as P

COLORS = 3
NEAR = 16
CAP = 2
AXES = ("gx", "gy")
VMEM_LIMIT = 62 * 1024 * 1024
MESH = pl.DeviceIdType.MESH


def split3(f):
    hi = f.astype(jnp.bfloat16).astype(jnp.float32)
    rest = f - hi
    mid = rest.astype(jnp.bfloat16).astype(jnp.float32)
    return hi, mid, rest - mid


def source_features(pos, m):
    lanes = pos.shape[1]
    sq = jnp.sum(pos * pos, axis=0, keepdims=True)
    d = -jnp.sum(m * pos, axis=0, keepdims=True)
    hi, mid, lo = split3(jnp.concatenate([pos, sq, m, d], axis=0))
    ones = jnp.ones((8, lanes), jnp.float32)
    half = jnp.concatenate([hi, hi, hi, mid, mid, lo, ones, jnp.zeros_like(ones)], axis=0)
    return jnp.concatenate([half, half], axis=0).T


def receiver_weights(pos, nrm):
    lanes = pos.shape[1]
    zero3 = jnp.zeros((3, lanes), jnp.float32)
    zero1 = jnp.zeros((1, lanes), jnp.float32)
    one1 = jnp.ones((1, lanes), jnp.float32)
    zero5 = jnp.zeros((5, lanes), jnp.float32)
    zero8 = jnp.zeros((8, lanes), jnp.float32)

    def column(feat, const):
        hi, mid, lo = split3(feat)
        chi, cmid, clo = split3(const)
        return jnp.concatenate(
            [hi, mid, lo, hi, mid, hi, jnp.concatenate([chi, cmid, clo, zero5], axis=0), zero8],
            axis=0,
        )

    dist = column(
        jnp.concatenate([-2.0 * pos, one1, zero3, zero1], axis=0),
        jnp.sum(pos * pos, axis=0, keepdims=True) + 1.0,
    )
    along_p = column(
        jnp.concatenate([nrm, zero1, zero3, zero1], axis=0),
        -jnp.sum(nrm * pos, axis=0, keepdims=True),
    )
    along_q = column(jnp.concatenate([zero3, zero1, pos, one1], axis=0), zero1)
    return jnp.concatenate([dist, along_p, along_q], axis=1)


def block_diag(w):
    z = jnp.zeros_like(w)
    return jnp.concatenate(
        [jnp.concatenate([w, z], axis=1), jnp.concatenate([z, w], axis=1)], axis=0
    ).astype(jnp.bfloat16)


def row_tiles(rows_ref, slot, base, weights, feats, tiles, side):
    v = tiles.shape[-1] // 2
    first = lax.broadcasted_iota(jnp.int32, (v, v), 1) < v // 2
    for i in range(rows_ref.shape[1] // 4):
        t = [rows_ref[slot, i * 4 + j] for j in range(4)]
        x = jnp.concatenate(
            [
                jnp.where(first, feats[t[0]], feats[t[1]]),
                jnp.where(first, feats[t[2]], feats[t[3]]),
            ],
            axis=0,
        )
        g = jnp.dot(x, weights, preferred_element_type=jnp.float32)
        for j in range(4):
            r, c = (j // 2) * v, (j % 2) * 3 * v
            dist = g[r : r + v, c : c + v]
            ap = g[r : r + v, c + v : c + 2 * v]
            aq = g[r : r + v, c + 2 * v : c + 3 * v]
            f = jnp.maximum(ap, 0.0) * jnp.maximum(aq, 0.0) / (dist * dist)
            at = base + (i * 4 + j) * v
            tiles[at : at + v, side * v : (side + 1) * v] = f.astype(jnp.bfloat16)


def contract(rows_ref, i, base, field, tiles):
    v = tiles.shape[-1] // 2
    count = rows_ref.shape[1]
    picked = jnp.concatenate(
        [
            jnp.concatenate([field[rows_ref[2 * i + side, j]] for j in range(count)], axis=1)
            for side in range(2)
        ],
        axis=0,
    )
    both = jnp.dot(
        picked, tiles[i, base : base + count * v, :], preferred_element_type=jnp.float32
    )
    rows = both.shape[0] // 2
    return both[0:rows, 0:v], both[rows:, v:]


def bounce_kernel(
    n, ny, ch, cuts,
    pairs, home, transfer, positions, normals, area, albedo,
    one_hbm, two_hbm, energy_ref,
    *scratch,
):
    (
        near_rows, far_ids, far_rows, low_s, req_s,
        tr, raw_pos, raw_nrm, raw_area, raw_alb, geo,
        wire_planes, guest_planes, wire, guest_wire, field,
        geo_own, geo_fwd, geo_in, near_feats, far_feats, wts, tiles,
        req_v, req_in, acc, one, two, out1, out2, en, en_in,
    ) = scratch[:32]
    k = len(cuts)
    groups = [scratch[32 + i * k : 32 + (i + 1) * k] for i in range(7)]
    box_own, box_fwd, box_in, box_in2, guest, planes_in, planes_in2 = groups
    loc, stat_s, stat_r, req_sems, en_sems = scratch[32 + 7 * k : 37 + 7 * k]
    peer_sems = scratch[37 + 7 * k :]
    bf16, f32, i32 = jnp.bfloat16, jnp.float32, jnp.int32

    gx, gy = lax.axis_index("gx"), lax.axis_index("gy")
    me = gx * ny + gy
    h, nh = ny // 2, n // 2
    side = lax.div(gy, h)
    mate_y = lax.rem(gy + h, ny)
    mate = gx * ny + mate_y
    spot = gx * h + gy - side * h
    b, v = area.shape
    near = near_rows.shape[1]
    far = far_ids.shape[1]

    def peer(d):
        t = lax.rem(me + d, n)
        return (lax.div(t, ny), lax.rem(t, ny))

    def side_peer(d):
        t = lax.rem(spot + d, nh)
        return t, (lax.div(t, h), side * h + lax.rem(t, h))

    def each(count, fn):
        def step(d, carry):
            fn(d)
            return carry

        lax.fori_loop(1, count, step, 0, unroll=5)

    def pair(ref, t):
        return ref.at[pl.ds(t * CAP, CAP)]

    class Spread:
        def __init__(self, sems, src, dst):
            self.sems, self.src, self.dst = sems, src, dst

        def copy(self, d):
            t, dev = side_peer(d)
            return pltpu.make_async_remote_copy(
                src_ref=self.src(t), dst_ref=self.dst,
                send_sem=self.sems.at[0, d], recv_sem=self.sems.at[1, d],
                device_id=dev, device_id_type=MESH,
            )

        def start(self):
            each(nh, lambda d: self.copy(d).start())

        def wait(self):
            each(nh, lambda d: self.copy(d).wait())

    def to_mate(i, src, dst):
        return pltpu.make_async_remote_copy(
            src_ref=src, dst_ref=dst, send_sem=stat_s.at[i], recv_sem=stat_r.at[i],
            device_id=(gx, mate_y), device_id_type=MESH,
        )

    def en_copy(d):
        return pltpu.make_async_remote_copy(
            src_ref=en, dst_ref=en_in.at[me],
            send_sem=en_sems.at[0, d], recv_sem=en_sems.at[1, d],
            device_id=peer(d), device_id_type=MESH,
        )

    req_x = Spread(req_sems, lambda t: req_v.at[0], req_in.at[spot])
    geo_x = [
        Spread(peer_sems[0], lambda t: geo_own.at[t], geo_in.at[me]),
        Spread(peer_sems[1], lambda t: geo_fwd.at[t], geo_in.at[mate]),
    ]

    def field_x(i, base, box):
        return [
            Spread(peer_sems[base], lambda t: pair(box_own[i], t), pair(box[i], me)),
            Spread(peer_sems[base + 1], lambda t: pair(box_fwd[i], t), pair(box[i], mate)),
        ]

    first_x = [field_x(i, 2 + 2 * i, box_in) for i in range(k)]
    second_x = [field_x(i, 2 + 2 * k + 2 * i, box_in2) for i in range(k)]
    tops = [min(hi, ch) for lo, hi in cuts]
    geo_m = to_mate(0, wire_planes, guest_planes)
    first_m = [
        to_mate(1 + i, tr.at[pl.ds(lo, tops[i] - lo)], planes_in[i])
        for i, (lo, hi) in enumerate(cuts)
    ]
    second_m = [
        to_mate(1 + k + i, out1.at[pl.ds(lo, tops[i] - lo)], planes_in2[i])
        for i, (lo, hi) in enumerate(cuts)
    ]

    barrier = pltpu.get_barrier_semaphore()
    each(n, lambda d: pl.semaphore_signal(barrier, inc=1, device_id=peer(d), device_id_type=MESH))
    loads = [
        pltpu.make_async_copy(src, dst, loc.at[i])
        for i, (src, dst) in enumerate(
            [
                (positions, raw_pos), (normals, raw_nrm), (area, raw_area),
                (albedo, raw_alb), (transfer, tr),
            ]
        )
    ]
    for cp in loads:
        cp.start()

    lanes = req_v.shape[2]
    floor = lax.broadcasted_iota(i32, (1, lanes), 1) * b

    def scan(s, carry):
        low, high = carry
        for j in range(near):
            near_rows[s, j] = lax.rem(home[pairs[s, j]], b)
        for j in range(far):
            t = home[pairs[s, near + j]]
            far_ids[s, j] = t
            x = t - floor
            ok = (x >= 0) & (x < b)
            low = jnp.minimum(low, jnp.where(ok, x, b - 1))
            high = jnp.maximum(high, jnp.where(ok, x, 0))
        return low, high

    low, high = lax.fori_loop(
        0, b, scan, (jnp.full((1, lanes), b - 1, i32), jnp.zeros((1, lanes), i32))
    )
    req_v[0] = low + high * b
    req_v[1] = low
    req_in[spot] = low + high * b
    low_cp = pltpu.make_async_copy(req_v.at[1], low_s, loc.at[5])
    low_cp.start()

    for cp in loads[:4]:
        cp.wait()
    m = raw_nrm[...] * (raw_area[...] * (1.0 / jnp.pi))[None]
    p_hi, p_mid, _ = split3(raw_pos[...])
    m_hi, m_mid, _ = split3(m)
    geo[...] = jnp.swapaxes(
        jnp.concatenate(
            [raw_pos[...], m, raw_nrm[...], raw_area[...][None], raw_alb[...],
             jnp.zeros((3, b, v), f32)], axis=0
        ),
        0, 1,
    )
    planes = jnp.concatenate([p_hi, p_mid, m_hi, m_mid], axis=0)
    wire_planes[...] = planes.astype(bf16)
    wire[...] = jnp.swapaxes(
        jnp.concatenate([planes, jnp.zeros((4, b, v), f32)], axis=0), 0, 1
    ).astype(bf16)
    loads[4].wait()

    def rows_of(source, i, base):
        lo, hi = cuts[i]
        part = source[lo - base : tops[i] - base]
        if hi > ch:
            part = jnp.concatenate([part, jnp.zeros((hi - ch, b, v), bf16)], axis=0)
        return jnp.swapaxes(part, 0, 1)

    for i, (lo, hi) in enumerate(cuts):
        field[:, lo:hi] = rows_of(tr, i, 0)

    def table(read, count, feats):
        def step(t, carry):
            for i in range(4):
                feats[t * 4 + i] = source_features(*read(t * 4 + i)).astype(bf16)
            return carry

        lax.fori_loop(0, count // 4, step, 0)

    table(lambda t: (geo[t, 0:3], geo[t, 3:6]), b, near_feats)

    def near_slots(lo, hi):
        def step(i, carry):
            for side in range(2):
                s = 2 * i + side
                w = block_diag(receiver_weights(geo[s, 0:3], geo[s, 6:9]))
                wts[s] = w
                row_tiles(near_rows, s, 0, w, near_feats, tiles.at[i], side)
            return carry

        lax.fori_loop(lo // 2, hi // 2, step, 0)

    pl.semaphore_wait(barrier, n - 1)
    req_x.start()
    for cp in [geo_m] + first_m[:1]:
        cp.start()
    near_slots(0, b // 4)
    for box in (geo_in,) + tuple(box_in) + tuple(box_in2):
        width = box.shape[0] // n
        for c in range(width):
            box[me * width + c] = jnp.zeros(box.shape[1:], box.dtype)
    req_x.wait()
    ask_cp = pltpu.make_async_copy(req_in, req_s, loc.at[0])
    ask_cp.start()
    ask_cp.wait()

    def asked(t, dev):
        r = req_s[t, 0, dev]
        hi = lax.div(r, b)
        return r - hi * b, hi

    def pack(dev, put):
        def step(t, carry):
            put(t, *asked(t, dev))
            return carry

        lax.fori_loop(0, nh, step, 0, unroll=4)

    def geo_pair(source, x, y):
        return jnp.concatenate([source[x, 0:12], source[y, 0:12]], axis=0)

    def send_geo(x, dev, source, out):
        def put(t, p, q):
            out[t] = geo_pair(source, p, q)

        pack(dev, put)
        x.start()

    def send_field(x, dev, read, out):
        def put(t, p, q):
            out[t * CAP] = read(p)
            out[t * CAP + 1] = read(q)

        pack(dev, put)
        x.start()

    def send_own(i, x, source):
        lo, hi = cuts[i]
        send_field(x[0], me, lambda t: source[t, lo:hi], box_own[i])

    def send_guest(i, x, m, source, box):
        m.wait()
        guest[i][...] = rows_of(source[i], i, cuts[i][0])
        send_field(x[1], mate, lambda t: guest[i][t], box_fwd[i])
        for c, t in enumerate(asked(spot, mate)):
            box[i][mate * CAP + c] = guest[i][t]

    send_geo(geo_x[0], me, wire, geo_own)
    geo_m.wait()
    guest_wire[...] = jnp.swapaxes(
        jnp.concatenate([guest_planes[...].astype(f32), jnp.zeros((4, b, v), f32)], axis=0), 0, 1
    ).astype(bf16)
    send_geo(geo_x[1], mate, guest_wire, geo_fwd)
    for cp in first_m[1:]:
        cp.start()
    geo_in[mate] = geo_pair(guest_wire, *asked(spot, mate))
    send_own(0, first_x[0], field)

    low_cp.wait()

    def far_index(s, carry):
        for j in range(far):
            t = far_ids[s, j]
            owner = lax.div(t, b)
            far_rows[s, j] = owner * CAP + (t - owner * b > low_s[0, owner]).astype(i32)
        return carry

    lax.fori_loop(0, b, far_index, 0)
    near_slots(b // 4, 3 * b // 4)
    near_slots(3 * b // 4, b)
    def near_sum(source):
        def step(i, carry):
            acc[2 * i], acc[2 * i + 1] = contract(near_rows, i, 0, source, tiles)
            return carry

        lax.fori_loop(0, b // 2, step, 0, unroll=4)

    near_sum(field)
    for x in geo_x:
        x.wait()
    send_guest(0, first_x[0], first_m[0], planes_in, box_in)
    for i in range(1, k):
        send_own(i, first_x[i], field)

    def far_geo(t):
        g = geo_in[t].astype(f32)
        return [(g[q : q + 3] + g[q + 3 : q + 6], g[q + 6 : q + 9] + g[q + 9 : q + 12]) for q in (0, 12)]

    def far_table(t, carry):
        for i in range(4):
            for c, g in enumerate(far_geo(t * 4 + i)):
                far_feats[(t * 4 + i) * CAP + c] = source_features(*g).astype(bf16)
        return carry

    lax.fori_loop(0, n // 4, far_table, 0)

    def far_slot(i, carry):
        for side in range(2):
            s = 2 * i + side
            row_tiles(far_rows, s, near * v, wts[s], far_feats, tiles.at[i], side)
        return carry

    lax.fori_loop(0, b // 8, far_slot, 0)
    for i in range(1, k):
        send_guest(i, first_x[i], first_m[i], planes_in, box_in)
    lax.fori_loop(b // 8, b // 2, far_slot, 0)

    def finish(i, box, write):
        lo, hi = cuts[i]
        row = lax.broadcasted_iota(i32, (hi - lo, v), 0) + lo

        def step(pair_id, e):
            sums = contract(far_rows, pair_id, near * v, box[i], tiles)
            for side in range(2):
                s = 2 * pair_id + side
                total = acc[s, lo:hi] + sums[side]
                shade = jnp.broadcast_to(geo[s, 12:13, :], (hi - lo, v))
                for c in range(COLORS - 2, -1, -1):
                    shade = jnp.where(
                        row < (c + 1) * (ch // COLORS), geo[s, 10 + c : 11 + c, :], shade
                    )
                val = total * shade
                keep = val if hi <= ch else jnp.where(row < ch, val, 0.0)
                write(s, lo, hi, val.astype(bf16))
                e = e + jnp.sum(keep * keep, axis=0, keepdims=True) * geo[s, 9:10, :]
            return e

        return lambda e: lax.fori_loop(0, b // 2, step, e, unroll=4)

    def to_planes(source, out, i):
        lo, hi = cuts[i]
        out[lo : tops[i]] = jnp.swapaxes(source[:, lo:hi], 0, 1)[0 : tops[i] - lo]

    def keep(ref):
        def write(s, lo, hi, val):
            ref[s, lo:hi] = val

        return write

    e1 = jnp.zeros((1, v), f32)
    for i in range(k):
        for x in first_x[i]:
            x.wait()
        e1 = finish(i, box_in, keep(one))(e1)
        to_planes(one, out1, i)
        second_m[i].start()
        send_own(i, second_x[i], one)
    one_cp = pltpu.make_async_copy(out1, one_hbm, loc.at[0])
    one_cp.start()
    send_guest(0, second_x[0], second_m[0], planes_in2, box_in2)
    near_sum(one)
    for i in range(1, k):
        send_guest(i, second_x[i], second_m[i], planes_in2, box_in2)
    e2 = jnp.zeros((1, v), f32)
    for i in range(k):
        for x in second_x[i]:
            x.wait()
        e2 = finish(i, box_in2, keep(two))(e2)
        if i < k - 1:
            to_planes(two, out2, i)
    en[...] = jnp.concatenate([e1, e2], axis=0)
    en_in[me] = en[...]
    each(n, lambda d: en_copy(d).start())
    to_planes(two, out2, k - 1)
    two_cp = pltpu.make_async_copy(out2, two_hbm, loc.at[1])
    two_cp.start()
    one_cp.wait()
    each(n, lambda d: en_copy(d).wait())
    total = jnp.sum(en_in[...], axis=0) * (1.0 / (n * b * v * ch))
    energy_ref[0] = jnp.sum(total[0:1])
    energy_ref[1] = jnp.sum(total[1:2])
    two_cp.wait()


def body(transfer, positions, normals, area, albedo, pairs, home):
    n = lax.axis_size(AXES)
    b, ch, v = transfer.shape
    far = pairs.shape[1] - NEAR
    rows = -(-ch // 16) * 16
    cut = 16
    cuts = ((0, cut), (cut, rows))
    bf16, f32, i32 = jnp.bfloat16, jnp.float32, jnp.int32
    lanes = -(-n // 128) * 128

    smem = pl.BlockSpec(memory_space=pltpu.SMEM)
    hbm = pl.BlockSpec(memory_space=pl.ANY)
    nh = n // 2
    sem = pltpu.SemaphoreType.DMA((2, nh))
    sizes = [hi - lo for lo, hi in cuts]
    boxes = [pltpu.VMEM((nh * CAP, size, v), bf16) for size in sizes] * 2
    boxes += [pltpu.VMEM((n * CAP, size, v), bf16) for size in sizes] * 2
    boxes += [pltpu.VMEM((b, size, v), bf16) for size in sizes]
    boxes += [pltpu.VMEM((min(hi, ch) - lo, b, v), bf16) for lo, hi in cuts] * 2
    one, two, energies = pl.pallas_call(
        functools.partial(bounce_kernel, n, lax.axis_size("gy"), ch, cuts),
        name="bounces",
        in_specs=[smem, smem] + [hbm] * 5,
        out_specs=[hbm, hbm, smem],
        out_shape=[
            jax.ShapeDtypeStruct((ch, b, v), bf16),
            jax.ShapeDtypeStruct((ch, b, v), bf16),
            jax.ShapeDtypeStruct((2,), f32),
        ],
        scratch_shapes=[
            pltpu.SMEM((b, NEAR), i32),
            pltpu.SMEM((b, far), i32),
            pltpu.SMEM((b, far), i32),
            pltpu.SMEM((1, lanes), i32),
            pltpu.SMEM((nh, 1, lanes), i32),
            pltpu.VMEM((ch, b, v), bf16),
            pltpu.VMEM((3, b, v), f32),
            pltpu.VMEM((3, b, v), f32),
            pltpu.VMEM((b, v), f32),
            pltpu.VMEM((3, b, v), f32),
            pltpu.VMEM((b, 16, v), f32),
            pltpu.VMEM((12, b, v), bf16),
            pltpu.VMEM((12, b, v), bf16),
            pltpu.VMEM((b, 16, v), bf16),
            pltpu.VMEM((b, 16, v), bf16),
            pltpu.VMEM((b, rows, v), bf16),
            pltpu.VMEM((nh, 24, v), bf16),
            pltpu.VMEM((nh, 24, v), bf16),
            pltpu.VMEM((n, 24, v), bf16),
            pltpu.VMEM((b, v, v), bf16),
            pltpu.VMEM((n * CAP, v, v), bf16),
            pltpu.VMEM((b, v, 6 * v), bf16),
            pltpu.VMEM((b // 2, (NEAR + far) * v, 2 * v), bf16),
            pltpu.VMEM((2, 1, lanes), i32),
            pltpu.VMEM((nh, 1, lanes), i32),
            pltpu.VMEM((b, rows, v), f32),
            pltpu.VMEM((b, rows, v), bf16),
            pltpu.VMEM((b, rows, v), bf16),
            pltpu.VMEM((ch, b, v), bf16),
            pltpu.VMEM((ch, b, v), bf16),
            pltpu.VMEM((2, v), f32),
            pltpu.VMEM((n, 2, v), f32),
        ]
        + boxes
        + [pltpu.SemaphoreType.DMA((6,))]
        + [pltpu.SemaphoreType.DMA((1 + 2 * len(cuts),))] * 2
        + [sem, pltpu.SemaphoreType.DMA((2, n))]
        + [sem] * (2 + 4 * len(cuts)),
        compiler_params=pltpu.CompilerParams(
            collective_id=0, has_side_effects=True, vmem_limit_bytes=VMEM_LIMIT
        ),
    )(
        pairs, home,
        jnp.swapaxes(transfer, 0, 1), jnp.swapaxes(positions, 0, 1),
        jnp.swapaxes(normals, 0, 1), area, jnp.swapaxes(albedo, 0, 1),
    )
    return jnp.swapaxes(one, 0, 1), jnp.swapaxes(two, 0, 1), energies


def solution(mesh):
    return jax.shard_map(
        body,
        mesh=mesh,
        in_specs=(
            P(AXES, None, None),
            P(AXES, None, None),
            P(AXES, None, None),
            P(AXES, None),
            P(AXES, None, None),
            P(AXES, None),
            P(),
        ),
        out_specs=(P(AXES, None, None), P(AXES, None, None), P()),
        check_vma=False,
    )
```

```python
import functools

import jax
import jax.numpy as jnp
from jax import lax
from jax.experimental import pallas as pl
from jax.experimental.pallas import tpu as pltpu
from jax.sharding import PartitionSpec as P

COLORS = 3
NEAR = 16
CAP = 2
AXES = ("gx", "gy")
VMEM_LIMIT = 62 * 1024 * 1024
MESH = pl.DeviceIdType.MESH


def split3(f):
    hi = f.astype(jnp.bfloat16).astype(jnp.float32)
    rest = f - hi
    mid = rest.astype(jnp.bfloat16).astype(jnp.float32)
    return hi, mid, rest - mid


def source_features(pos, m):
    lanes = pos.shape[1]
    sq = jnp.sum(pos * pos, axis=0, keepdims=True)
    d = -jnp.sum(m * pos, axis=0, keepdims=True)
    hi, mid, lo = split3(jnp.concatenate([pos, sq, m, d], axis=0))
    ones = jnp.ones((8, lanes), jnp.float32)
    half = jnp.concatenate([hi, hi, hi, mid, mid, lo, ones, jnp.zeros_like(ones)], axis=0)
    return jnp.concatenate([half, half], axis=0).T


def receiver_weights(pos, nrm):
    lanes = pos.shape[1]
    zero3 = jnp.zeros((3, lanes), jnp.float32)
    zero1 = jnp.zeros((1, lanes), jnp.float32)
    one1 = jnp.ones((1, lanes), jnp.float32)
    zero5 = jnp.zeros((5, lanes), jnp.float32)
    zero8 = jnp.zeros((8, lanes), jnp.float32)

    def column(feat, const):
        hi, mid, lo = split3(feat)
        chi, cmid, clo = split3(const)
        return jnp.concatenate(
            [hi, mid, lo, hi, mid, hi, jnp.concatenate([chi, cmid, clo, zero5], axis=0), zero8],
            axis=0,
        )

    dist = column(
        jnp.concatenate([-2.0 * pos, one1, zero3, zero1], axis=0),
        jnp.sum(pos * pos, axis=0, keepdims=True) + 1.0,
    )
    along_p = column(
        jnp.concatenate([nrm, zero1, zero3, zero1], axis=0),
        -jnp.sum(nrm * pos, axis=0, keepdims=True),
    )
    along_q = column(jnp.concatenate([zero3, zero1, pos, one1], axis=0), zero1)
    return jnp.concatenate([dist, along_p, along_q], axis=1)


def block_diag(w):
    z = jnp.zeros_like(w)
    return jnp.concatenate(
        [jnp.concatenate([w, z], axis=1), jnp.concatenate([z, w], axis=1)], axis=0
    ).astype(jnp.bfloat16)


def row_tiles(rows_ref, slot, base, weights, feats, tiles, side):
    v = tiles.shape[-1] // 2
    first = lax.broadcasted_iota(jnp.int32, (v, v), 1) < v // 2
    for i in range(rows_ref.shape[1] // 4):
        t = [rows_ref[slot, i * 4 + j] for j in range(4)]
        x = jnp.concatenate(
            [
                jnp.where(first, feats[t[0]], feats[t[1]]),
                jnp.where(first, feats[t[2]], feats[t[3]]),
            ],
            axis=0,
        )
        g = jnp.dot(x, weights, preferred_element_type=jnp.float32)
        for j in range(4):
            r, c = (j // 2) * v, (j % 2) * 3 * v
            dist = g[r : r + v, c : c + v]
            ap = g[r : r + v, c + v : c + 2 * v]
            aq = g[r : r + v, c + 2 * v : c + 3 * v]
            f = jnp.maximum(ap, 0.0) * jnp.maximum(aq, 0.0) / (dist * dist)
            at = base + (i * 4 + j) * v
            tiles[at : at + v, side * v : (side + 1) * v] = f.astype(jnp.bfloat16)


def contract(rows_ref, i, base, field, tiles):
    v = tiles.shape[-1] // 2
    count = rows_ref.shape[1]
    picked = jnp.concatenate(
        [
            jnp.concatenate([field[rows_ref[2 * i + side, j]] for j in range(count)], axis=1)
            for side in range(2)
        ],
        axis=0,
    )
    both = jnp.dot(
        picked, tiles[i, base : base + count * v, :], preferred_element_type=jnp.float32
    )
    rows = both.shape[0] // 2
    return both[0:rows, 0:v], both[rows:, v:]


def bounce_kernel(
    n, ny, ch, cuts,
    pairs, home, transfer, positions, normals, area, albedo,
    one_hbm, two_hbm, energy_ref,
    *scratch,
):
    (
        near_rows, far_ids, far_rows, low_s, req_s,
        tr, raw_pos, raw_nrm, raw_area, raw_alb, geo,
        wire_planes, guest_planes, wire, guest_wire, field,
        geo_own, geo_fwd, geo_in, near_feats, far_feats, wts, tiles,
        req_v, req_in, acc, one, two, out1, out2, en, en_in,
    ) = scratch[:32]
    k = len(cuts)
    groups = [scratch[32 + i * k : 32 + (i + 1) * k] for i in range(7)]
    box_own, box_fwd, box_in, box_in2, guest, planes_in, planes_in2 = groups
    loc, stat_s, stat_r, req_sems, en_sems = scratch[32 + 7 * k : 37 + 7 * k]
    peer_sems = scratch[37 + 7 * k :]
    bf16, f32, i32 = jnp.bfloat16, jnp.float32, jnp.int32

    gx, gy = lax.axis_index("gx"), lax.axis_index("gy")
    me = gx * ny + gy
    h, nh = ny // 2, n // 2
    side = lax.div(gy, h)
    mate_y = lax.rem(gy + h, ny)
    mate = gx * ny + mate_y
    spot = gx * h + gy - side * h
    b, v = area.shape
    near = near_rows.shape[1]
    far = far_ids.shape[1]

    def peer(d):
        t = lax.rem(me + d, n)
        return (lax.div(t, ny), lax.rem(t, ny))

    def side_peer(d):
        t = lax.rem(spot + d, nh)
        return t, (lax.div(t, h), side * h + lax.rem(t, h))

    def each(count, fn):
        def step(d, carry):
            fn(d)
            return carry

        lax.fori_loop(1, count, step, 0, unroll=5)

    def pair(ref, t):
        return ref.at[pl.ds(t * CAP, CAP)]

    class Spread:
        def __init__(self, sems, src, dst):
            self.sems, self.src, self.dst = sems, src, dst

        def copy(self, d):
            t, dev = side_peer(d)
            return pltpu.make_async_remote_copy(
                src_ref=self.src(t), dst_ref=self.dst,
                send_sem=self.sems.at[0, d], recv_sem=self.sems.at[1, d],
                device_id=dev, device_id_type=MESH,
            )

        def start(self):
            each(nh, lambda d: self.copy(d).start())

        def wait(self):
            each(nh, lambda d: self.copy(d).wait())

    def to_mate(i, src, dst):
        return pltpu.make_async_remote_copy(
            src_ref=src, dst_ref=dst, send_sem=stat_s.at[i], recv_sem=stat_r.at[i],
            device_id=(gx, mate_y), device_id_type=MESH,
        )

    def en_copy(d):
        return pltpu.make_async_remote_copy(
            src_ref=en, dst_ref=en_in.at[me],
            send_sem=en_sems.at[0, d], recv_sem=en_sems.at[1, d],
            device_id=peer(d), device_id_type=MESH,
        )

    req_x = Spread(req_sems, lambda t: req_v.at[0], req_in.at[spot])
    geo_x = [
        Spread(peer_sems[0], lambda t: geo_own.at[t], geo_in.at[me]),
        Spread(peer_sems[1], lambda t: geo_fwd.at[t], geo_in.at[mate]),
    ]

    def field_x(i, base, box):
        return [
            Spread(peer_sems[base], lambda t: pair(box_own[i], t), pair(box[i], me)),
            Spread(peer_sems[base + 1], lambda t: pair(box_fwd[i], t), pair(box[i], mate)),
        ]

    first_x = [field_x(i, 2 + 2 * i, box_in) for i in range(k)]
    second_x = [field_x(i, 2 + 2 * k + 2 * i, box_in2) for i in range(k)]
    tops = [min(hi, ch) for lo, hi in cuts]
    geo_m = to_mate(0, wire_planes, guest_planes)
    first_m = [
        to_mate(1 + i, tr.at[pl.ds(lo, tops[i] - lo)], planes_in[i])
        for i, (lo, hi) in enumerate(cuts)
    ]
    second_m = [
        to_mate(1 + k + i, out1.at[pl.ds(lo, tops[i] - lo)], planes_in2[i])
        for i, (lo, hi) in enumerate(cuts)
    ]

    barrier = pltpu.get_barrier_semaphore()
    each(n, lambda d: pl.semaphore_signal(barrier, inc=1, device_id=peer(d), device_id_type=MESH))
    loads = [
        pltpu.make_async_copy(src, dst, loc.at[i])
        for i, (src, dst) in enumerate(
            [
                (positions, raw_pos), (normals, raw_nrm), (area, raw_area),
                (albedo, raw_alb), (transfer, tr),
            ]
        )
    ]
    for cp in loads:
        cp.start()

    lanes = req_v.shape[2]
    floor = lax.broadcasted_iota(i32, (1, lanes), 1) * b

    def scan(s, carry):
        low, high = carry
        for j in range(near):
            near_rows[s, j] = lax.rem(home[pairs[s, j]], b)
        for j in range(far):
            t = home[pairs[s, near + j]]
            far_ids[s, j] = t
            x = t - floor
            ok = (x >= 0) & (x < b)
            low = jnp.minimum(low, jnp.where(ok, x, b - 1))
            high = jnp.maximum(high, jnp.where(ok, x, 0))
        return low, high

    low, high = lax.fori_loop(
        0, b, scan, (jnp.full((1, lanes), b - 1, i32), jnp.zeros((1, lanes), i32))
    )
    req_v[0] = low + high * b
    req_v[1] = low
    req_in[spot] = low + high * b
    low_cp = pltpu.make_async_copy(req_v.at[1], low_s, loc.at[5])
    low_cp.start()

    for cp in loads[:4]:
        cp.wait()
    m = raw_nrm[...] * (raw_area[...] * (1.0 / jnp.pi))[None]
    p_hi, p_mid, _ = split3(raw_pos[...])
    m_hi, m_mid, _ = split3(m)
    geo[...] = jnp.swapaxes(
        jnp.concatenate(
            [raw_pos[...], m, raw_nrm[...], raw_area[...][None], raw_alb[...],
             jnp.zeros((3, b, v), f32)], axis=0
        ),
        0, 1,
    )
    planes = jnp.concatenate([p_hi, p_mid, m_hi, m_mid], axis=0)
    wire_planes[...] = planes.astype(bf16)
    wire[...] = jnp.swapaxes(
        jnp.concatenate([planes, jnp.zeros((4, b, v), f32)], axis=0), 0, 1
    ).astype(bf16)
    loads[4].wait()

    def rows_of(source, i, base):
        lo, hi = cuts[i]
        part = source[lo - base : tops[i] - base]
        if hi > ch:
            part = jnp.concatenate([part, jnp.zeros((hi - ch, b, v), bf16)], axis=0)
        return jnp.swapaxes(part, 0, 1)

    for i, (lo, hi) in enumerate(cuts):
        field[:, lo:hi] = rows_of(tr, i, 0)

    def table(read, count, feats):
        def step(t, carry):
            for i in range(4):
                feats[t * 4 + i] = source_features(*read(t * 4 + i)).astype(bf16)
            return carry

        lax.fori_loop(0, count // 4, step, 0)

    table(lambda t: (geo[t, 0:3], geo[t, 3:6]), b, near_feats)

    def near_slots(lo, hi):
        def step(i, carry):
            for side in range(2):
                s = 2 * i + side
                w = block_diag(receiver_weights(geo[s, 0:3], geo[s, 6:9]))
                wts[s] = w
                row_tiles(near_rows, s, 0, w, near_feats, tiles.at[i], side)
            return carry

        lax.fori_loop(lo // 2, hi // 2, step, 0)

    pl.semaphore_wait(barrier, n - 1)
    req_x.start()
    for cp in [geo_m] + first_m[:1]:
        cp.start()
    near_slots(0, b // 4)
    for box in (geo_in,) + tuple(box_in) + tuple(box_in2):
        width = box.shape[0] // n
        for c in range(width):
            box[me * width + c] = jnp.zeros(box.shape[1:], box.dtype)
    req_x.wait()
    ask_cp = pltpu.make_async_copy(req_in, req_s, loc.at[0])
    ask_cp.start()
    ask_cp.wait()

    def asked(t, dev):
        r = req_s[t, 0, dev]
        hi = lax.div(r, b)
        return r - hi * b, hi

    def pack(dev, put):
        def step(t, carry):
            put(t, *asked(t, dev))
            return carry

        lax.fori_loop(0, nh, step, 0, unroll=4)

    def geo_pair(source, x, y):
        return jnp.concatenate([source[x, 0:12], source[y, 0:12]], axis=0)

    def send_geo(x, dev, source, out):
        def put(t, p, q):
            out[t] = geo_pair(source, p, q)

        pack(dev, put)
        x.start()

    def send_field(x, dev, read, out):
        def put(t, p, q):
            out[t * CAP] = read(p)
            out[t * CAP + 1] = read(q)

        pack(dev, put)
        x.start()

    def send_own(i, x, source):
        lo, hi = cuts[i]
        send_field(x[0], me, lambda t: source[t, lo:hi], box_own[i])

    def send_guest(i, x, m, source, box):
        m.wait()
        guest[i][...] = rows_of(source[i], i, cuts[i][0])
        send_field(x[1], mate, lambda t: guest[i][t], box_fwd[i])
        for c, t in enumerate(asked(spot, mate)):
            box[i][mate * CAP + c] = guest[i][t]

    send_geo(geo_x[0], me, wire, geo_own)
    geo_m.wait()
    guest_wire[...] = jnp.swapaxes(
        jnp.concatenate([guest_planes[...].astype(f32), jnp.zeros((4, b, v), f32)], axis=0), 0, 1
    ).astype(bf16)
    send_geo(geo_x[1], mate, guest_wire, geo_fwd)
    for cp in first_m[1:]:
        cp.start()
    geo_in[mate] = geo_pair(guest_wire, *asked(spot, mate))
    send_own(0, first_x[0], field)

    low_cp.wait()

    def far_index(s, carry):
        for j in range(far):
            t = far_ids[s, j]
            owner = lax.div(t, b)
            far_rows[s, j] = owner * CAP + (t - owner * b > low_s[0, owner]).astype(i32)
        return carry

    lax.fori_loop(0, b, far_index, 0)
    near_slots(b // 4, 3 * b // 4)
    near_slots(3 * b // 4, b)
    def near_sum(source):
        def step(i, carry):
            acc[2 * i], acc[2 * i + 1] = contract(near_rows, i, 0, source, tiles)
            return carry

        lax.fori_loop(0, b // 2, step, 0, unroll=4)

    near_sum(field)
    for x in geo_x:
        x.wait()
    send_guest(0, first_x[0], first_m[0], planes_in, box_in)
    for i in range(1, k):
        send_own(i, first_x[i], field)

    def far_geo(t):
        g = geo_in[t].astype(f32)
        return [(g[q : q + 3] + g[q + 3 : q + 6], g[q + 6 : q + 9] + g[q + 9 : q + 12]) for q in (0, 12)]

    def far_table(t, carry):
        for i in range(8):
            for c, g in enumerate(far_geo(t * 8 + i)):
                far_feats[(t * 8 + i) * CAP + c] = source_features(*g).astype(bf16)
        return carry

    lax.fori_loop(0, n // 8, far_table, 0)

    def far_slot(i, carry):
        for side in range(2):
            s = 2 * i + side
            row_tiles(far_rows, s, near * v, wts[s], far_feats, tiles.at[i], side)
        return carry

    lax.fori_loop(0, b // 8, far_slot, 0)
    for i in range(1, k):
        send_guest(i, first_x[i], first_m[i], planes_in, box_in)
    lax.fori_loop(b // 8, b // 2, far_slot, 0)

    def finish(i, box, write):
        lo, hi = cuts[i]
        row = lax.broadcasted_iota(i32, (hi - lo, v), 0) + lo

        def step(pair_id, e):
            sums = contract(far_rows, pair_id, near * v, box[i], tiles)
            for side in range(2):
                s = 2 * pair_id + side
                total = acc[s, lo:hi] + sums[side]
                shade = jnp.broadcast_to(geo[s, 12:13, :], (hi - lo, v))
                for c in range(COLORS - 2, -1, -1):
                    shade = jnp.where(
                        row < (c + 1) * (ch // COLORS), geo[s, 10 + c : 11 + c, :], shade
                    )
                val = total * shade
                keep = val if hi <= ch else jnp.where(row < ch, val, 0.0)
                write(s, lo, hi, val.astype(bf16))
                e = e + jnp.sum(keep * keep, axis=0, keepdims=True) * geo[s, 9:10, :]
            return e

        return lambda e: lax.fori_loop(0, b // 2, step, e, unroll=4)

    def to_planes(source, out, i):
        lo, hi = cuts[i]
        out[lo : tops[i]] = jnp.swapaxes(source[:, lo:hi], 0, 1)[0 : tops[i] - lo]

    def keep(ref):
        def write(s, lo, hi, val):
            ref[s, lo:hi] = val

        return write

    e1 = jnp.zeros((1, v), f32)
    for i in range(k):
        for x in first_x[i]:
            x.wait()
        e1 = finish(i, box_in, keep(one))(e1)
        to_planes(one, out1, i)
        second_m[i].start()
        send_own(i, second_x[i], one)
    one_cp = pltpu.make_async_copy(out1, one_hbm, loc.at[0])
    one_cp.start()
    send_guest(0, second_x[0], second_m[0], planes_in2, box_in2)
    near_sum(one)
    for i in range(1, k):
        send_guest(i, second_x[i], second_m[i], planes_in2, box_in2)
    e2 = jnp.zeros((1, v), f32)
    for i in range(k):
        for x in second_x[i]:
            x.wait()
        e2 = finish(i, box_in2, keep(two))(e2)
        if i < k - 1:
            to_planes(two, out2, i)
    en[...] = jnp.concatenate([e1, e2], axis=0)
    en_in[me] = en[...]
    each(n, lambda d: en_copy(d).start())
    to_planes(two, out2, k - 1)
    two_cp = pltpu.make_async_copy(out2, two_hbm, loc.at[1])
    two_cp.start()
    one_cp.wait()
    each(n, lambda d: en_copy(d).wait())
    total = jnp.sum(en_in[...], axis=0) * (1.0 / (n * b * v * ch))
    energy_ref[0] = jnp.sum(total[0:1])
    energy_ref[1] = jnp.sum(total[1:2])
    two_cp.wait()


def body(transfer, positions, normals, area, albedo, pairs, home):
    n = lax.axis_size(AXES)
    b, ch, v = transfer.shape
    far = pairs.shape[1] - NEAR
    rows = -(-ch // 16) * 16
    cut = 16
    cuts = ((0, cut), (cut, rows))
    bf16, f32, i32 = jnp.bfloat16, jnp.float32, jnp.int32
    lanes = -(-n // 128) * 128

    smem = pl.BlockSpec(memory_space=pltpu.SMEM)
    hbm = pl.BlockSpec(memory_space=pl.ANY)
    nh = n // 2
    sem = pltpu.SemaphoreType.DMA((2, nh))
    sizes = [hi - lo for lo, hi in cuts]
    boxes = [pltpu.VMEM((nh * CAP, size, v), bf16) for size in sizes] * 2
    boxes += [pltpu.VMEM((n * CAP, size, v), bf16) for size in sizes] * 2
    boxes += [pltpu.VMEM((b, size, v), bf16) for size in sizes]
    boxes += [pltpu.VMEM((min(hi, ch) - lo, b, v), bf16) for lo, hi in cuts] * 2
    one, two, energies = pl.pallas_call(
        functools.partial(bounce_kernel, n, lax.axis_size("gy"), ch, cuts),
        name="bounces",
        in_specs=[smem, smem] + [hbm] * 5,
        out_specs=[hbm, hbm, smem],
        out_shape=[
            jax.ShapeDtypeStruct((ch, b, v), bf16),
            jax.ShapeDtypeStruct((ch, b, v), bf16),
            jax.ShapeDtypeStruct((2,), f32),
        ],
        scratch_shapes=[
            pltpu.SMEM((b, NEAR), i32),
            pltpu.SMEM((b, far), i32),
            pltpu.SMEM((b, far), i32),
            pltpu.SMEM((1, lanes), i32),
            pltpu.SMEM((nh, 1, lanes), i32),
            pltpu.VMEM((ch, b, v), bf16),
            pltpu.VMEM((3, b, v), f32),
            pltpu.VMEM((3, b, v), f32),
            pltpu.VMEM((b, v), f32),
            pltpu.VMEM((3, b, v), f32),
            pltpu.VMEM((b, 16, v), f32),
            pltpu.VMEM((12, b, v), bf16),
            pltpu.VMEM((12, b, v), bf16),
            pltpu.VMEM((b, 16, v), bf16),
            pltpu.VMEM((b, 16, v), bf16),
            pltpu.VMEM((b, rows, v), bf16),
            pltpu.VMEM((nh, 24, v), bf16),
            pltpu.VMEM((nh, 24, v), bf16),
            pltpu.VMEM((n, 24, v), bf16),
            pltpu.VMEM((b, v, v), bf16),
            pltpu.VMEM((n * CAP, v, v), bf16),
            pltpu.VMEM((b, v, 6 * v), bf16),
            pltpu.VMEM((b // 2, (NEAR + far) * v, 2 * v), bf16),
            pltpu.VMEM((2, 1, lanes), i32),
            pltpu.VMEM((nh, 1, lanes), i32),
            pltpu.VMEM((b, rows, v), f32),
            pltpu.VMEM((b, rows, v), bf16),
            pltpu.VMEM((b, rows, v), bf16),
            pltpu.VMEM((ch, b, v), bf16),
            pltpu.VMEM((ch, b, v), bf16),
            pltpu.VMEM((2, v), f32),
            pltpu.VMEM((n, 2, v), f32),
        ]
        + boxes
        + [pltpu.SemaphoreType.DMA((6,))]
        + [pltpu.SemaphoreType.DMA((1 + 2 * len(cuts),))] * 2
        + [sem, pltpu.SemaphoreType.DMA((2, n))]
        + [sem] * (2 + 4 * len(cuts)),
        compiler_params=pltpu.CompilerParams(
            collective_id=0, has_side_effects=True, vmem_limit_bytes=VMEM_LIMIT
        ),
    )(
        pairs, home,
        jnp.swapaxes(transfer, 0, 1), jnp.swapaxes(positions, 0, 1),
        jnp.swapaxes(normals, 0, 1), area, jnp.swapaxes(albedo, 0, 1),
    )
    return jnp.swapaxes(one, 0, 1), jnp.swapaxes(two, 0, 1), energies


def solution(mesh):
    return jax.shard_map(
        body,
        mesh=mesh,
        in_specs=(
            P(AXES, None, None),
            P(AXES, None, None),
            P(AXES, None, None),
            P(AXES, None),
            P(AXES, None, None),
            P(AXES, None),
            P(),
        ),
        out_specs=(P(AXES, None, None), P(AXES, None, None), P()),
        check_vma=False,
    )
```
